32 devices in a mesh: dp: 4 (over x, core), pipe: 2 (over y), tensor: 4 (over z).
Axes of the slice: x: 2, y: 2, z: 4, core: 2. Of those that a mesh axis runs over, the one named last changes fastest.
Arguments:
- weights: bfloat16 [2816, 1408], P(('dp', 'pipe', 'tensor')), may hold values from -6 to 6
- first_moment: bfloat16 [2816, 1408], P(('dp', 'pipe', 'tensor')), may hold values from -6 to 6
- second_moment: bfloat16 [2816, 1408], P(('dp', 'pipe', 'tensor')), may hold values from 0.049804688 to 5
- row_weight: float32 [1408], replicated, may hold values from -1 to 1
- col_weight: float32 [1408], replicated, may hold values from 1 to 4
Outputs:
- weight_tiles: bfloat16 [2816, 1408], P(('pipe', 'tensor'))
- first_tiles: bfloat16 [2816, 1408], P(('pipe', 'tensor'))
- second_tiles: bfloat16 [2816, 1408], P(('pipe', 'tensor'))
- checksums: float32 [3, 2, 4, 11], P(None, 'pipe', 'tensor')
The draws below stay inside these ranges and needn't reach their ends.
All inputs are finite; a program needn't handle non-finite values.
Results may differ from the reference program's by a relative error of at most 0.001.
Values may be sent and summed in bfloat16 or wider, within the bound.
No kernel may reach another device: no remote copies, remote signals or barrier semaphores. Data moves between devices by JAX's collectives and lax.ppermute only.
A program may use at most 64 MiB of HBM per device.

```python
import math
import jax
import jax.numpy as jnp
from jax import lax

D = 1408
CHECK_COLS = 128
BLOCKS = 2
N_TENSOR = 4


def block_scale(key, dims, shards, low, high):
    gain = 1.0
    for position, blocks in shards:
        heights = jax.random.uniform(jax.random.fold_in(jax.random.fold_in(key, 6), position), (blocks,), jnp.float32, low / len(shards), high / len(shards))
        gain = gain * jnp.repeat(jnp.exp(heights), dims[position] // blocks).reshape((-1,) + (1,) * (len(dims) - 1 - position))
    return gain


def scatter_about(stream_key, dims, width, bound, pieces=(), kind=jnp.bfloat16):
    values = width * jax.random.normal(stream_key, dims, jnp.float32)
    if pieces:
        values = values * block_scale(stream_key, dims, pieces, -0.22, 0.18)
    return jnp.clip(values, -bound, bound).astype(kind)


def setup_inputs(seed: int = 0) -> dict:
    seeds = jax.random.split(jax.random.key(seed), 6)
    return {
        "weights": scatter_about(seeds[0], (BLOCKS * D, D), 1.0, 6.0, ((0, 32),)),
        "first_moment": scatter_about(seeds[1], (BLOCKS * D, D), 1.0, 6.0, ((0, 32),)),
        "second_moment": jnp.clip(jnp.exp(math.log(5.0) - 4.609084 * jax.random.uniform(seeds[2], (BLOCKS * D, D), jnp.float32) ** block_scale(seeds[2], (BLOCKS * D, D), ((0, 32),), -0.2, 0.2)), 0.049804688, 5.0).astype(jnp.bfloat16),
        "row_weight": jnp.clip(jax.random.uniform(seeds[3], (D,), jnp.float32, -1.0, 1.0), -1.0, 1.0),
        "col_weight": jnp.clip(jnp.exp(jax.random.uniform(seeds[4], (D,), jnp.float32, math.log(1.0), math.log(4.0))), 1.0, 4.0),
    }


def reference(weights, first_moment, second_moment, row_weight, col_weight):
    tile_rows = D // N_TENSOR
    col_blocks = D // CHECK_COLS
    factor = float(tile_rows * CHECK_COLS) ** -0.5
    row_grid = row_weight.reshape(N_TENSOR, tile_rows)
    col_grid = col_weight.reshape(col_blocks, CHECK_COLS)

    def one_kind(data):
        blocked = data.astype(jnp.float32).reshape(BLOCKS, N_TENSOR, tile_rows, col_blocks, CHECK_COLS)
        weighted = jnp.einsum("bjrce,jr->bjce", blocked, row_grid, precision=lax.Precision.HIGHEST)
        return factor * jnp.sum(weighted * col_grid, axis=3)

    checks = jnp.stack([one_kind(weights), one_kind(first_moment), one_kind(second_moment)]).astype(jnp.float32)
    return weights, first_moment, second_moment, checks
```

```python
import jax
import jax.numpy as jnp
from jax import lax
from jax.sharding import PartitionSpec as P

CHECK_COLS = 128
AXES = ("dp", "pipe", "tensor")


def shard_moves(dp_count, pipe_count, tensor_count):
    moves = []
    for flat in range(dp_count * pipe_count * tensor_count):
        tile, shard = divmod(flat, dp_count)
        moves.append((flat, shard * pipe_count * tensor_count + tile))
    return moves


def column_sums(tile, row_part, col_weight, col_blocks):
    row_mixed = jnp.dot(
        row_part[None, :], tile.astype(jnp.float32), precision=lax.Precision.HIGHEST
    )[0]
    return jnp.sum((row_mixed * col_weight).reshape(col_blocks, -1), axis=1)


def shards(weights, first_moment, second_moment, row_weight, col_weight):
    dp_count = lax.axis_size("dp")
    pipe_count = lax.axis_size("pipe")
    tensor_count = lax.axis_size("tensor")
    shard_rows, width = weights.shape
    tile_rows = shard_rows * dp_count
    col_blocks = width // CHECK_COLS
    factor = float(tile_rows * CHECK_COLS) ** (-0.5)
    moves = shard_moves(dp_count, pipe_count, tensor_count)
    arrived = [
        lax.ppermute(item, AXES, moves) for item in (weights, first_moment, second_moment)
    ]
    tiles = [lax.all_gather(item, "dp", axis=0, tiled=True) for item in arrived]
    row_part = lax.dynamic_slice_in_dim(
        row_weight, lax.axis_index("tensor") * tile_rows, tile_rows
    )
    checks = jnp.stack([column_sums(tile, row_part, col_weight, col_blocks) for tile in tiles])
    return (*tiles, checks[:, None, None, :] * factor)


def solution(mesh):
    return jax.shard_map(
        shards,
        mesh=mesh,
        in_specs=(P(AXES, None), P(AXES, None), P(AXES, None), P(), P()),
        out_specs=(
            P(("pipe", "tensor"), None),
            P(("pipe", "tensor"), None),
            P(("pipe", "tensor"), None),
            P(None, "pipe", "tensor", None),
        ),
        check_vma=False,
    )
```

```python
import jax
import jax.numpy as jnp
from jax import lax
from jax.experimental import pallas as pl
from jax.experimental.pallas import tpu as pltpu
from jax.sharding import PartitionSpec as P

CHECK_COLS = 128
AXES = ("dp", "pipe", "tensor")
CORES = 2
ROW_ALIGN = 8


class Routes:
    def __init__(self, dp_count, pipe_count, tensor_count):
        self.dp, self.pipe, self.tensor = dp_count, pipe_count, tensor_count
        self.columns = dp_count // CORES

    def device(self, column, core, section, tensor):
        return ((column * CORES + core) * self.pipe + section) * self.tensor + tensor

    def shards(self):
        for flat in range(self.dp * self.pipe * self.tensor):
            tile, shard = divmod(flat, self.dp)
            yield flat, *divmod(tile, self.tensor), shard

    def shift(self, tile):
        return tile * self.columns // self.tensor

    def home(self, shard, tile):
        return (shard + self.shift(tile)) % self.columns, shard // self.columns

    def direct(self):
        moves = []
        for flat, section, tile, shard in self.shards():
            column, core = self.home(shard, tile)
            moves.append((flat, self.device(column, core, section, tile)))
        return moves

    def two_step(self, turn):
        first, second, filled = [], [], {}
        for flat, section, tile, shard in self.shards():
            column, core = self.home(shard, tile)
            column = (column + turn) % self.columns
            stop = (column, section, flat % self.tensor)
            slot = filled.get(stop, 0)
            filled[stop] = slot + 1
            middle = self.device(column, slot, section, flat % self.tensor)
            first.append((flat, middle))
            second.append((middle, self.device(column, core, section, tile)))
        return first, second

    def turned(self, turn):
        step = turn * CORES * self.pipe * self.tensor
        total = self.dp * self.pipe * self.tensor
        return [(flat, (flat + step) % total) for flat in range(total)]

    def core_swap(self):
        per = self.pipe * self.tensor
        return [
            (dp * per + rest, (dp ^ 1) * per + rest) for dp in range(self.dp) for rest in range(per)
        ]

    def fits(self, shard_rows):
        if shard_rows % ROW_ALIGN or self.dp % CORES or self.dp % self.tensor:
            return False
        first, _ = self.two_step(0)
        return len({target for _, target in first}) == len(first)


def finish_tile(pieces, starts, row_part, col_weight, factor, earlier, last):
    shard_rows, width = pieces[0].shape
    count = len(pieces)
    col_blocks = width // CHECK_COLS

    def kernel(starts_ref, rows_ref, cols_ref, *refs):
        piece_refs = refs[:count]
        earlier_refs = refs[count : count + len(earlier)]
        tile_ref, check_ref, sems = refs[count + len(earlier) :]
        copies = []
        for i, piece in enumerate(piece_refs):
            start = pl.multiple_of(starts_ref[i], ROW_ALIGN)
            copy = pltpu.make_async_copy(piece, tile_ref.at[pl.ds(start, shard_rows)], sems.at[i])
            copy.start()
            copies.append(copy)
        total = jnp.zeros((ROW_ALIGN, width), jnp.float32)
        for i, piece in enumerate(piece_refs):
            start = pl.multiple_of(starts_ref[i], ROW_ALIGN)
            weighted = piece[...].astype(jnp.float32) * rows_ref[pl.ds(start, shard_rows), :]
            total += jnp.sum(weighted.reshape(-1, ROW_ALIGN, width), axis=0)
        mixed = jnp.sum(total, axis=0, keepdims=True) * cols_ref[...] * factor
        sums = jnp.concatenate(
            [
                jnp.sum(mixed[:, c * CHECK_COLS : (c + 1) * CHECK_COLS], axis=1, keepdims=True)
                for c in range(col_blocks)
            ],
            axis=1,
        )
        if last:
            for k, ref in enumerate(earlier_refs):
                check_ref[k, 0] = ref[...]
            check_ref[len(earlier), 0] = sums
        else:
            check_ref[...] = sums
        for copy in copies:
            copy.wait()

    check_shape = (len(earlier) + 1, 1, 1, col_blocks) if last else (1, col_blocks)
    vmem = pl.BlockSpec(memory_space=pltpu.VMEM)
    return pl.pallas_call(
        kernel,
        out_shape=(
            jax.ShapeDtypeStruct((shard_rows * count, width), pieces[0].dtype),
            jax.ShapeDtypeStruct(check_shape, jnp.float32),
        ),
        in_specs=[pl.BlockSpec(memory_space=pltpu.SMEM)] + [vmem] * (2 + count + len(earlier)),
        out_specs=(pl.BlockSpec(memory_space=pl.ANY), vmem),
        scratch_shapes=[pltpu.SemaphoreType.DMA((count,))],
    )(starts, row_part, col_weight, *pieces, *earlier)


def column_sums(tile, row_part, col_weight, col_blocks):
    row_mixed = jnp.dot(
        row_part[None, :], tile.astype(jnp.float32), precision=lax.Precision.HIGHEST
    )[0]
    return jnp.sum((row_mixed * col_weight).reshape(col_blocks, -1), axis=1)


def gathered(routes, sources, row_part, col_weight, factor):
    per = routes.pipe * routes.tensor
    moves = [
        (flat, shard * per + section * routes.tensor + tile)
        for flat, section, tile, shard in routes.shards()
    ]
    tiles = [
        lax.all_gather(lax.ppermute(item, AXES, moves), "dp", axis=0, tiled=True)
        for item in sources
    ]
    col_blocks = col_weight.shape[0] // CHECK_COLS
    checks = jnp.stack([column_sums(tile, row_part, col_weight, col_blocks) for tile in tiles])
    return (*tiles, checks[:, None, None, :] * factor)


def named(scope, item, moves):
    with jax.named_scope(scope):
        return lax.ppermute(item, AXES, moves)


def permuted(routes, sources, row_part, col_weight, factor):
    columns = routes.columns
    shard_rows = sources[0].shape[0]
    swap = routes.core_swap()
    direct = routes.direct()
    two = [routes.two_step(turn) for turn in range(columns)]
    weights, first_moment, second_moment = sources

    def spread(tag, mine):
        held = [mine] + [
            named(f"{tag}_turn{turn}", mine, routes.turned(turn)) for turn in range(1, columns)
        ]
        return held + [named(f"{tag}_swap{k}", item, swap) for k, item in enumerate(held)]

    pieces0 = spread("a", named("a_direct", weights, direct))
    middle = named("b_plane", first_moment, two[0][0])
    pieces1 = spread("b", named("b_line", middle, two[0][1]))
    held = []
    for turn, (first, second) in enumerate(two):
        middle = named(f"c_plane{turn}", second_moment, first)
        held.append(named(f"c_line{turn}", middle, second))
    pieces2 = held + [named(f"c_swap{k}", item, swap) for k, item in enumerate(held)]

    column, core = lax.axis_index("dp") // CORES, lax.axis_index("dp") % CORES
    shift = lax.axis_index("tensor") * columns // routes.tensor
    turns = jnp.arange(columns)
    from_column = (column - turns - shift) % columns
    starts = jnp.concatenate(
        [(core * columns + from_column), ((1 - core) * columns + from_column)]
    )
    starts = (starts * shard_rows).astype(jnp.int32)
    rows = row_part[:, None]
    cols = col_weight[None, :]
    tile0, check0 = finish_tile(pieces0, starts, rows, cols, factor, (), False)
    tile1, check1 = finish_tile(pieces1, starts, rows, cols, factor, (), False)
    tile2, checks = finish_tile(pieces2, starts, rows, cols, factor, (check0, check1), True)
    return tile0, tile1, tile2, checks


def shards(weights, first_moment, second_moment, row_weight, col_weight):
    routes = Routes(lax.axis_size("dp"), lax.axis_size("pipe"), lax.axis_size("tensor"))
    shard_rows = weights.shape[0]
    tile_rows = shard_rows * routes.dp
    factor = float(tile_rows * CHECK_COLS) ** (-0.5)
    row_part = lax.dynamic_slice_in_dim(
        row_weight, lax.axis_index("tensor") * tile_rows, tile_rows
    )
    sources = (weights, first_moment, second_moment)
    plan = permuted if routes.fits(shard_rows) else gathered
    return plan(routes, sources, row_part, col_weight, factor)


def solution(mesh):
    return jax.shard_map(
        shards,
        mesh=mesh,
        in_specs=(P(AXES, None), P(AXES, None), P(AXES, None), P(), P()),
        out_specs=(
            P(("pipe", "tensor"), None),
            P(("pipe", "tensor"), None),
            P(("pipe", "tensor"), None),
            P(None, "pipe", "tensor", None),
        ),
        check_vma=False,
    )
```

```python
import itertools

import jax
import jax.numpy as jnp
from jax import lax
from jax.experimental import pallas as pl
from jax.experimental.pallas import tpu as pltpu
from jax.sharding import PartitionSpec as P


CHECK_COLS = 128
AXES = ("dp", "pipe", "tensor")
CORES = 2
ROW_ALIGN = 8
KERNEL_VMEM = 8 * 2**20


PLANS = ("D", "P", "B")
TURNS = (0, 0, 0)
CUT = (0, 8)
CALLS = (((0, "all"),), ((1, "early"), (2, "early")), ((1, "late"), (2, "late")))


class Routes:
    def __init__(self, dp_count, pipe_count, tensor_count):
        self.dp, self.pipe, self.tensor = dp_count, pipe_count, tensor_count
        self.per_dp = pipe_count * tensor_count
        self.total = dp_count * self.per_dp
        self.columns = dp_count // CORES

    def goal(self, flat):
        tile, shard = divmod(flat, self.dp)
        return (*divmod(tile, self.tensor), shard)

    def column(self, flat, turn):
        _, tile, shard = self.goal(flat)
        return (shard + tile + tile * self.columns // self.tensor + turn) % self.columns

    def place(self, chips):
        arriving = {}
        for source, chip in chips.items():
            arriving.setdefault(chip, []).append(source)
        placed = {}
        for (column, section, tensor), sources in arriving.items():
            base = column * CORES * self.per_dp + section * self.tensor + tensor
            targets = [base + core * self.per_dp for core in range(CORES)]
            if len(sources) != CORES:
                return None
            best = min(
                itertools.permutations(targets),
                key=lambda some: (
                    sum(source == target for source, target in zip(sources, some)),
                    sum((source - target) // self.per_dp % CORES for source, target in zip(sources, some)),
                ),
            )
            placed.update(zip(sources, best))
        return placed

    def direct(self, turn):
        chips = {}
        for flat in range(self.total):
            section, tile, _ = self.goal(flat)
            chips[flat] = (self.column(flat, turn), section, tile)
        return self.place(chips)

    def two_step(self, turn):
        chips = {}
        for flat in range(self.total):
            chips[flat] = (self.column(flat, turn), self.goal(flat)[0], flat % self.tensor)
        first = self.place(chips)
        if first is None:
            return None, None
        chips = {}
        for flat, middle in first.items():
            section, tile, _ = self.goal(flat)
            chips[middle] = (self.column(flat, turn), section, tile)
        return first, self.place(chips)

    def mixed(self):
        chips, rows = {}, {}
        for flat in range(self.total):
            dp, rest = divmod(flat, self.per_dp)
            row = (rest // self.tensor + dp + rest) % self.pipe
            rows[flat] = row
            chips[flat] = (dp // CORES, row, flat % self.tensor)
        first = self.place(chips)
        if first is None:
            return None
        chips = {}
        for flat, middle in first.items():
            chips[middle] = (middle // self.per_dp // CORES, rows[flat], self.goal(flat)[1])
        second = self.place(chips)
        if second is None:
            return None
        lasts = []
        for turn in range(self.columns):
            chips = {}
            for flat, middle in first.items():
                section, tile, shard = self.goal(flat)
                chips[second[middle]] = ((shard // self.columns + turn) % self.columns, section, tile)
            lasts.append(self.place(chips))
        return first, second, lasts

    def turned(self, turn):
        step = turn * CORES * self.per_dp
        return {flat: (flat + step) % self.total for flat in range(self.total)}

    def core_swap(self):
        return {flat: self.swapped(flat) for flat in range(self.total)}

    def swapped(self, flat):
        dp, rest = divmod(flat, self.per_dp)
        return (dp ^ 1) * self.per_dp + rest

    def fits(self, shard_rows):
        if shard_rows % ROW_ALIGN or self.dp % CORES or self.dp % self.tensor:
            return False
        return None not in (self.direct(0), *self.two_step(0), self.mixed())


def shard_starts(held, flat, routes, shard_rows):
    bits = max(1, (routes.dp - 1).bit_length())
    per_word = 30 // bits
    start = 0
    for word in range(-(-routes.total // per_word)):
        first = word * per_word
        packed = sum(
            held[first + k] << (bits * k) for k in range(min(per_word, routes.total - first))
        )
        place = jnp.clip(flat - first, 0, per_word - 1)
        found = lax.shift_right_logical(jnp.int32(packed), (place * bits).astype(jnp.int32))
        here = jnp.logical_and(flat >= first, flat < first + per_word)
        start = jnp.where(here, found & ((1 << bits) - 1), start)
    return start * shard_rows


def place_pieces(routes, shard_rows, jobs, tiles, partials, rows, cols, factor, complete, last):
    width, dtype = jobs[0][1][0].shape[1], jobs[0][1][0].dtype
    col_blocks = width // CHECK_COLS
    arrays = sorted({array for _, _, parts in jobs for array, _, _ in parts})
    begun = sorted(partials) if last else [array for array in arrays if array in partials]
    into = [array for array in arrays if array in tiles]
    count = sum(len(pieces) * len(parts) for _, pieces, parts in jobs)

    def kernel(*refs):
        refs = list(refs)
        take = lambda n: [refs.pop(0) for _ in range(n)]
        rows_ref, cols_ref = take(2)
        job_refs = [take(len(pieces)) for _, pieces, _ in jobs]
        begun_refs = dict(zip(begun, take(len(begun))))
        take(len(into))
        tile_refs = dict(zip(arrays, take(len(arrays))))
        check_refs = take(1) if last else take(len(arrays))
        sems = refs.pop(0)
        index = lax.axis_index("tensor")
        flat = (lax.axis_index("dp") * routes.pipe + lax.axis_index("pipe")) * routes.tensor + index
        copies, blocks = [], []
        for (held, _, parts), piece_refs in zip(jobs, job_refs):
            for some, piece in zip(held, piece_refs):
                start = shard_starts(some, flat, routes, shard_rows)
                offset = 0
                for array, row, rows_here in parts:
                    first = pl.multiple_of(start + row, ROW_ALIGN)
                    source = piece.at[pl.ds(offset, rows_here)]
                    place = tile_refs[array].at[pl.ds(first, rows_here)]
                    copies.append(pltpu.make_async_copy(source, place, sems.at[len(copies)]))
                    copies[-1].start()
                    blocks.append((array, source, first))
                    offset += rows_here
        totals = {}
        for array in arrays:
            if array in begun_refs:
                totals[array] = [begun_refs[array][c] for c in range(col_blocks)]
            else:
                totals[array] = [jnp.zeros((ROW_ALIGN, CHECK_COLS), jnp.float32)] * col_blocks
        for array, source, first in blocks:
            weight_row = pl.multiple_of(index * shard_rows * routes.dp + first, ROW_ALIGN)
            part = rows_ref[pl.ds(weight_row, source.shape[0]), :]
            for c in range(col_blocks):
                block = source[:, c * CHECK_COLS : (c + 1) * CHECK_COLS]
                weighted = block.astype(jnp.float32) * part
                totals[array][c] += jnp.sum(weighted.reshape(-1, ROW_ALIGN, CHECK_COLS), axis=0)

        def checksums(some):
            sums = [
                jnp.sum(
                    jnp.sum(total, axis=0, keepdims=True) * cols_ref[c : c + 1, :],
                    axis=1,
                    keepdims=True,
                )
                for c, total in enumerate(some)
            ]
            return jnp.concatenate(sums, axis=1) * factor

        if last:
            sums_ref = refs.pop(0)
            for array in sorted({*arrays, *begun}):
                sums_ref[array, 0] = checksums(totals[array]) if array in totals else begun_refs[array][...]
            copies.append(pltpu.make_async_copy(sums_ref, check_refs[0], sems.at[len(copies)]))
            copies[-1].start()
        else:
            for ref, array in zip(check_refs, arrays):
                if array in complete:
                    ref[...] = checksums(totals[array])
                else:
                    for c in range(col_blocks):
                        ref[c] = totals[array][c]
        for copy in copies:
            copy.wait()

    vmem, anywhere = pl.BlockSpec(memory_space=pltpu.VMEM), pl.BlockSpec(memory_space=pl.ANY)
    scratch = [pltpu.SemaphoreType.DMA((count + 1,))]
    tile_shape = jax.ShapeDtypeStruct((shard_rows * routes.dp, width), dtype)
    if last:
        check_shape = jax.ShapeDtypeStruct((len({*arrays, *begun}), 1, 1, col_blocks), jnp.float32)
        scratch.append(pltpu.VMEM(check_shape.shape, jnp.float32))
        check_shapes, check_specs = [check_shape], [anywhere]
    else:
        shapes = [
            (1, col_blocks) if array in complete else (col_blocks, ROW_ALIGN, CHECK_COLS)
            for array in arrays
        ]
        check_shapes = [jax.ShapeDtypeStruct(shape, jnp.float32) for shape in shapes]
        check_specs = [vmem] * len(arrays)
    inputs = [rows, cols, *(piece for _, pieces, _ in jobs for piece in pieces)]
    inputs += [partials[array] for array in begun]
    out = pl.pallas_call(
        kernel,
        out_shape=[tile_shape] * len(arrays) + check_shapes,
        in_specs=[vmem] * len(inputs) + [anywhere] * len(into),
        out_specs=[anywhere] * len(arrays) + check_specs,
        scratch_shapes=scratch,
        input_output_aliases={len(inputs) + i: arrays.index(k) for i, k in enumerate(into)},
        compiler_params=pltpu.CompilerParams(vmem_limit_bytes=KERNEL_VMEM),
    )(*inputs, *(tiles[array] for array in into))
    tiles.update(zip(arrays, out))
    if last:
        return out[-1]
    partials.update(zip(arrays, out[len(arrays) :]))


def column_sums(tile, row_part, col_weight, col_blocks):
    row_mixed = jnp.dot(
        row_part[None, :], tile.astype(jnp.float32), precision=lax.Precision.HIGHEST
    )[0]
    return jnp.sum((row_mixed * col_weight).reshape(col_blocks, -1), axis=1)


def gathered(routes, sources, row_weight, col_weight, factor):
    moves = {}
    for flat in range(routes.total):
        section, tile, shard = routes.goal(flat)
        moves[flat] = shard * routes.per_dp + section * routes.tensor + tile
    tiles = [
        lax.all_gather(lax.ppermute(item, AXES, list(moves.items())), "dp", axis=0, tiled=True)
        for item in sources
    ]
    tile_rows = tiles[0].shape[0]
    row_part = lax.dynamic_slice_in_dim(
        row_weight, lax.axis_index("tensor") * tile_rows, tile_rows
    )
    col_blocks = col_weight.shape[0] // CHECK_COLS
    checks = jnp.stack([column_sums(tile, row_part, col_weight, col_blocks) for tile in tiles])
    return (*tiles, checks[:, None, None, :] * factor)


def named(item, moves):
    return lax.ppermute(item, AXES, list(moves.items()))


def move_array(routes, item, plan, turn):
    columns = routes.columns
    if plan == "B":
        turns = [turn + k for k in range(columns)]
    else:
        turns = [turn]
    held, pieces = [], []
    if plan == "Q":
        first, second, lasts = routes.mixed()
        item = named(named(item, first), second)
        for some in lasts:
            pieces.append(named(item, some))
            held.append({some[second[first[flat]]]: routes.goal(flat)[2] for flat in first})
        turns = []
    for way in turns:
        if plan == "D":
            placed = routes.direct(way)
            pieces.append(named(item, placed))
        else:
            first, second = routes.two_step(way)
            middle = named(item, first)
            pieces.append(named(middle, second))
            placed = {flat: second[first[flat]] for flat in first}
        held.append({target: routes.goal(flat)[2] for flat, target in placed.items()})
    if plan in "DP":
        for k in range(1, columns):
            moves = routes.turned(k)
            pieces.append(named(pieces[0], moves))
            held.append({target: held[0][source] for source, target in moves.items()})
    swap = routes.core_swap()
    for k in range(len(pieces)):
        pieces.append(named(pieces[k], swap))
        held.append({target: held[k][source] for source, target in swap.items()})
    return held, pieces


def permuted(routes, sources, row_weight, col_weight, factor):
    rows = jnp.broadcast_to(row_weight[:, None], (row_weight.shape[0], CHECK_COLS))
    cols = col_weight.reshape(-1, CHECK_COLS)
    shard_rows = sources[0].shape[0]
    cut = shard_rows * CUT[0] // CUT[1] // ROW_ALIGN * ROW_ALIGN
    chunks = [[(0, 0, shard_rows)], [(1, 0, shard_rows), (2, 0, cut)], [(2, cut, shard_rows - cut)]]
    if cut == 0:
        chunks[1].pop()
    moved = []
    for parts, plan, turn in zip(chunks, PLANS, TURNS):
        items = [sources[array][row : row + count] for array, row, count in parts]
        item = items[0] if len(items) == 1 else jnp.concatenate(items)
        moved.append((*move_array(routes, item, plan, turn), parts))
    tiles, partials = {}, {}
    for number, call in enumerate(CALLS):
        jobs = []
        for k, half in call:
            held, pieces, parts = moved[k]
            late = [i for i in range(len(pieces)) if (i + 1) % routes.columns == 0]
            chosen = [i for i in range(len(pieces)) if half == "all" or (i in late) == (half == "late")]
            jobs.append(([held[i] for i in chosen], [pieces[i] for i in chosen], parts))
        later = [moved[k][2] for call in CALLS[number + 1 :] for k, _ in call]
        unfinished = {array for parts in later for array, _, _ in parts}
        complete = [array for array in range(len(sources)) if array not in unfinished]
        last = not later
        checks = place_pieces(
            routes, shard_rows, jobs, tiles, partials, rows, cols, factor, complete, last
        )
    return (tiles[0], tiles[1], tiles[2], checks)


def shards(weights, first_moment, second_moment, row_weight, col_weight):
    routes = Routes(lax.axis_size("dp"), lax.axis_size("pipe"), lax.axis_size("tensor"))
    shard_rows = weights.shape[0]
    tile_rows = shard_rows * routes.dp
    factor = float(tile_rows * CHECK_COLS) ** (-0.5)
    sources = (weights, first_moment, second_moment)
    plan = permuted if routes.fits(shard_rows) else gathered
    return plan(routes, sources, row_weight, col_weight, factor)


def solution(mesh):
    return jax.shard_map(
        shards,
        mesh=mesh,
        in_specs=(P(AXES, None), P(AXES, None), P(AXES, None), P(), P()),
        out_specs=(
            P(("pipe", "tensor"), None),
            P(("pipe", "tensor"), None),
            P(("pipe", "tensor"), None),
            P(None, "pipe", "tensor", None),
        ),
        check_vma=False,
    )
```
